32 devices in a mesh: grid: 8 (over z, x), band: 4 (over y, core).
Axes of the slice: x: 2, y: 2, z: 4, core: 2. Of those that a mesh axis runs over, the one named last changes fastest.
Arguments:
- basis: float32 [2048, 8192], P('band', 'grid'), as said below
- panel: float32 [1024, 8192], P('band', 'grid'), may hold values from -6 to 6
Outputs:
- new_panel: float32 [1024, 8192], P('band', 'grid')
- coeffs: float32 [2048, 1024], P('band')
The draws below stay inside these ranges and needn't reach their ends.
Inputs may be any that keep to these rules, and one draw needn't show every extreme that they name: The rows of basis are orthogonal to each other, each with squared sum 8192 (to float32 rounding).
All inputs are finite; a program needn't handle non-finite values.
Results may differ from the reference program's by a relative error of at most 0.000073.
Values sent between devices are 32-bit elements; how exact they have to be, the bound alone decides.
A program may use at most 128 MiB of HBM per device.

```python
import jax
import jax.numpy as jnp
from jax import lax

NQ = 2048
NP = 1024
NG = 8192


def draw_basis(key, part):
    sample = jax.random.normal(key, (NG, NQ), jnp.float32)
    ortho, upper = jnp.linalg.qr(sample)
    return (ortho.T * jnp.sqrt(jnp.float32(NG))).astype(jnp.float32)


def shard_levels(key, dims, split, least, high):
    def one(axis_at, blocks):
        steps = jax.random.uniform(jax.random.fold_in(jax.random.fold_in(key, 6), axis_at), (blocks,), jnp.float32, least / len(split), high / len(split))
        return jnp.repeat(jnp.exp(steps), dims[axis_at] // blocks).reshape((-1,) + (1,) * (len(dims) - axis_at - 1))

    loudness = one(*split[0])
    for cut in split[1:]:
        loudness = loudness * one(*cut)
    return loudness


def noise(key, shape, width, bound, shards=(), kind=jnp.bfloat16):
    array = jax.random.normal(key, shape, jnp.float32) * width
    if len(shards) > 0:
        array = shard_levels(key, shape, shards, -0.22, 0.18) * array
    return jnp.clip(array, min=-bound, max=bound).astype(kind)


def setup_inputs(seed: int = 0) -> dict:
    key_list = jax.random.split(jax.random.key(seed), 3)
    basis = draw_basis(jax.random.fold_in(key_list[2], 71), 0)
    panel = noise(key_list[1], (NP, NG), 1.0, 6.0, ((0, 4), (1, 8)), jnp.float32)
    return dict(basis=basis, panel=panel)


def reference(basis, panel):
    highest = lax.Precision.HIGHEST
    n_grid = basis.shape[1]
    coeffs = jnp.dot(basis, panel.T, precision=highest) / n_grid
    projected = panel - jnp.dot(coeffs.T, basis, precision=highest)
    gram = jnp.dot(projected, projected.T, precision=highest) / n_grid
    factor = jnp.linalg.cholesky(gram)
    new_panel = lax.linalg.triangular_solve(factor, projected, left_side=True, lower=True)
    return (new_panel, coeffs)
```

```python
import functools

import jax
import jax.numpy as jnp
from jax import lax
from jax.experimental import pallas as pl
from jax.experimental.pallas import tpu as pltpu
from jax.sharding import PartitionSpec as P

BLOCK = 128
ROWS = 8


def tdot(left, right):
    return lax.dot_general(
        left,
        right,
        (((1,), (1,)), ((), ())),
        precision=lax.Precision.HIGH,
        preferred_element_type=jnp.float32,
    )


def cdot(left, right):
    return lax.dot_general(
        left,
        right,
        (((0,), (0,)), ((), ())),
        precision=lax.Precision.HIGH,
        preferred_element_type=jnp.float32,
    )


def halves(x):
    high = x.astype(jnp.bfloat16)
    low = (x - high.astype(jnp.float32)).astype(jnp.bfloat16)
    return high, low


def left_parts(x):
    high, low = halves(x)
    return jnp.concatenate([high, high, low], 1)


def right_parts(x, axis):
    high, low = halves(x)
    return jnp.concatenate([high, low, high], axis)


def dot_nt(left, right):
    return lax.dot_general(
        left, right, (((1,), (1,)), ((), ())), preferred_element_type=jnp.float32
    )


def block_inverse(tiles):
    lanes = lax.broadcasted_iota(jnp.int32, (ROWS, BLOCK), 1)
    subs = lax.broadcasted_iota(jnp.int32, (ROWS, BLOCK), 0)
    shape = (ROWS, BLOCK)
    tiles = list(tiles)
    count = len(tiles)
    done = []
    for t in range(count):
        tile = tiles[t]
        base = ROWS * t
        here = (lanes >= base) & (lanes < base + ROWS)
        cols = [jnp.broadcast_to(tile[:, base + q : base + q + 1], shape) for q in range(ROWS)]
        entry = {
            (p, q): jnp.broadcast_to(cols[q][p : p + 1, :], shape)
            for q in range(ROWS)
            for p in range(q, ROWS)
        }
        start = jnp.where(here, jnp.where(lanes - base == subs, 1.0, 0.0), tile)
        rows = [jnp.broadcast_to(start[p : p + 1, :], shape) for p in range(ROWS)]
        unit = {}
        root = []
        scaled = []
        for q in range(ROWS):
            inv_root = lax.rsqrt(entry[q, q])
            inv = inv_root * inv_root
            root.append(inv_root)
            scaled.append(inv)
            for p in range(q + 1, ROWS):
                unit[p, q] = entry[p, q] * inv
            for p in range(q + 1, ROWS):
                for s in range(q + 1, p + 1):
                    entry[p, s] = entry[p, s] - unit[p, q] * entry[s, q]
                rows[p] = rows[p] - unit[p, q] * rows[q]
        out = rows[0] * root[0]
        for p in range(1, ROWS):
            out = jnp.where(subs == p, rows[p] * root[p], out)
        done.append(jnp.where(lanes <= base + subs, out, 0.0))
        if t + 1 < count:
            back = [rows[p] * scaled[p] for p in range(ROWS)]
            for p in range(ROWS - 1, 0, -1):
                for q in range(p):
                    back[q] = back[q] - unit[p, q] * back[p]
            for u in range(t + 1, count):
                old = tiles[u]
                new = jnp.where(here, 0.0, old)
                for p in range(ROWS):
                    new = new - jnp.broadcast_to(old[:, base + p : base + p + 1], shape) * back[p]
                tiles[u] = new
    return done


def factor_kernel(gram_ref, out_ref, diag_ref, right_ref):
    blocks = out_ref.shape[0] // BLOCK
    out_ref[...] = gram_ref[...]

    def step(k, carry):
        at = pl.ds(pl.multiple_of(k * BLOCK, BLOCK), BLOCK)
        base = pl.multiple_of(k * BLOCK, BLOCK)
        tiles = [
            out_ref[pl.ds(base + ROWS * t, ROWS), at] for t in range(BLOCK // ROWS)
        ]
        for t, tile in enumerate(block_inverse(tiles)):
            diag_ref[pl.ds(ROWS * t, ROWS), :] = tile
        diag = diag_ref[...]
        panel = jnp.dot(
            left_parts(diag),
            right_parts(out_ref[at, :], 0),
            preferred_element_type=jnp.float32,
        )
        out_ref[at, :] = panel
        out_ref[at, at] = diag
        right_ref[...] = right_parts(out_ref[at, :], 0)
        diag_right = right_parts(diag, 1)

        def update(i, carry):
            rows = pl.ds(pl.multiple_of(i * BLOCK, BLOCK), BLOCK)
            lower = dot_nt(left_parts(out_ref[rows, at]), diag_right)
            out_ref[rows, at] = jnp.zeros((BLOCK, BLOCK), jnp.float32)
            out_ref[rows, :] -= jnp.dot(
                left_parts(lower), right_ref[...], preferred_element_type=jnp.float32
            )
            return carry

        lax.fori_loop(k + 1, blocks, update, 0)
        return carry

    lax.fori_loop(0, blocks, step, 0)
    row = lax.broadcasted_iota(jnp.int32, (BLOCK, out_ref.shape[1]), 0)
    col = lax.broadcasted_iota(jnp.int32, (BLOCK, out_ref.shape[1]), 1)

    def clear(i, carry):
        rows = pl.ds(pl.multiple_of(i * BLOCK, BLOCK), BLOCK)
        out_ref[rows, :] = jnp.where(col <= row + i * BLOCK, out_ref[rows, :], 0.0)
        return carry

    lax.fori_loop(0, blocks, clear, 0)


def inverse_factor(gram):
    n = gram.shape[0]
    return pl.pallas_call(
        factor_kernel,
        out_shape=jax.ShapeDtypeStruct((n, n), jnp.float32),
        in_specs=[pl.BlockSpec(memory_space=pltpu.VMEM)],
        out_specs=pl.BlockSpec(memory_space=pltpu.VMEM),
        scratch_shapes=[
            pltpu.VMEM((BLOCK, BLOCK), jnp.float32),
            pltpu.VMEM((3 * BLOCK, n), jnp.bfloat16),
        ],
        compiler_params=pltpu.CompilerParams(vmem_limit_bytes=32 * 1024 * 1024),
        cost_estimate=pl.CostEstimate(
            flops=60 * n * n * n, bytes_accessed=8 * n * n, transcendentals=n
        ),
    )(gram)


def body(basis, panel):
    grid, band = lax.axis_size("grid"), lax.axis_size("band")
    n_grid = panel.shape[1] * grid
    rows_q = basis.shape[0]
    rows_p = panel.shape[0]
    n_panel = rows_p * band
    share_q, share_p = rows_q // grid, rows_p // grid
    panel_all = lax.all_gather(panel, "band", axis=0, tiled=True)
    stacked = jnp.concatenate(
        [basis.reshape(grid, share_q, -1), panel.reshape(grid, share_p, -1)], 1
    ).reshape(rows_q + rows_p, -1)
    both = tdot(stacked, panel_all)
    mine = lax.psum_scatter(both, "grid", scatter_dimension=0, tiled=True) / n_grid
    coeffs = lax.all_gather(mine[:share_q], "grid", axis=0, tiled=True)
    picked = lax.dynamic_index_in_dim(
        coeffs.reshape(rows_q, band, grid, share_p), lax.axis_index("grid"), 2, keepdims=False
    ).reshape(rows_q, band * share_p)
    square = lax.psum_scatter(cdot(picked, coeffs), "band", scatter_dimension=0, tiled=True)
    gram = lax.all_gather(
        mine[share_q:] - square, ("band", "grid"), axis=0, tiled=True
    )
    part = cdot(coeffs, basis)
    part, gram = lax.optimization_barrier((part, gram))
    removed = lax.psum(part, "band")
    inverse = inverse_factor(gram)
    inverse_rows = lax.dynamic_slice_in_dim(
        inverse, lax.axis_index("band") * rows_p, rows_p, 0
    )
    new_panel = jnp.dot(inverse_rows, panel_all - removed, precision=lax.Precision.HIGH)
    return (new_panel, coeffs)


def solution(mesh):
    placed = (P("band", "grid"), P("band", "grid"))
    return jax.shard_map(
        body,
        mesh=mesh,
        in_specs=placed,
        out_specs=(P("band", "grid"), P("band", None)),
        check_vma=False,
    )
```

```python
import functools

import jax
import jax.numpy as jnp
from jax import lax
from jax.experimental import pallas as pl
from jax.experimental.pallas import tpu as pltpu
from jax.sharding import PartitionSpec as P

BLOCK = 128
ROWS = 8


def tdot(left, right):
    return lax.dot_general(
        left,
        right,
        (((1,), (1,)), ((), ())),
        precision=lax.Precision.HIGH,
        preferred_element_type=jnp.float32,
    )


def cdot(left, right):
    return lax.dot_general(
        left,
        right,
        (((0,), (0,)), ((), ())),
        precision=lax.Precision.HIGH,
        preferred_element_type=jnp.float32,
    )


def halves(x):
    high = x.astype(jnp.bfloat16)
    low = (x - high.astype(jnp.float32)).astype(jnp.bfloat16)
    return high, low


def left_parts(x):
    high, low = halves(x)
    return jnp.concatenate([high, high, low], 1)


def right_parts(x, axis):
    high, low = halves(x)
    return jnp.concatenate([high, low, high], axis)


def dot_nt(left, right):
    return lax.dot_general(
        left, right, (((1,), (1,)), ((), ())), preferred_element_type=jnp.float32
    )


def block_inverse(tiles):
    lanes = lax.broadcasted_iota(jnp.int32, (ROWS, BLOCK), 1)
    subs = lax.broadcasted_iota(jnp.int32, (ROWS, BLOCK), 0)
    shape = (ROWS, BLOCK)
    tiles = list(tiles)
    count = len(tiles)
    done = []
    for t in range(count):
        tile = tiles[t]
        base = ROWS * t
        here = (lanes >= base) & (lanes < base + ROWS)
        cols = [jnp.broadcast_to(tile[:, base + q : base + q + 1], shape) for q in range(ROWS)]
        entry = {
            (p, q): jnp.broadcast_to(cols[q][p : p + 1, :], shape)
            for q in range(ROWS)
            for p in range(q, ROWS)
        }
        start = jnp.where(here, jnp.where(lanes - base == subs, 1.0, 0.0), tile)
        rows = [jnp.broadcast_to(start[p : p + 1, :], shape) for p in range(ROWS)]
        unit = {}
        root = []
        scaled = []
        for q in range(ROWS):
            inv_root = lax.rsqrt(entry[q, q])
            inv = inv_root * inv_root
            root.append(inv_root)
            scaled.append(inv)
            for p in range(q + 1, ROWS):
                unit[p, q] = entry[p, q] * inv
            for p in range(q + 1, ROWS):
                for s in range(q + 1, p + 1):
                    entry[p, s] = entry[p, s] - unit[p, q] * entry[s, q]
                rows[p] = rows[p] - unit[p, q] * rows[q]
        out = rows[0] * root[0]
        for p in range(1, ROWS):
            out = jnp.where(subs == p, rows[p] * root[p], out)
        done.append(jnp.where(lanes <= base + subs, out, 0.0))
        if t + 1 < count:
            back = [rows[p] * scaled[p] for p in range(ROWS)]
            for p in range(ROWS - 1, 0, -1):
                for q in range(p):
                    back[q] = back[q] - unit[p, q] * back[p]
            for u in range(t + 1, count):
                old = tiles[u]
                new = jnp.where(here, 0.0, old)
                for p in range(ROWS):
                    new = new - jnp.broadcast_to(old[:, base + p : base + p + 1], shape) * back[p]
                tiles[u] = new
    return done


def factor_kernel(gram_ref, out_ref, diag_ref, right_ref):
    blocks = out_ref.shape[0] // BLOCK
    for pair in range(blocks // 2):
        rows = slice(pair * BLOCK, (pair + 1) * BLOCK)
        for row, tiles, first in ((pair, pair + 1, 0), (blocks - 1 - pair, blocks - pair, pair + 1)):
            for col in range(tiles):
                tile = gram_ref[rows, (first + col) * BLOCK : (first + col + 1) * BLOCK]
                out_ref[row * BLOCK : (row + 1) * BLOCK, col * BLOCK : (col + 1) * BLOCK] = tile
                if col < row:
                    out_ref[col * BLOCK : (col + 1) * BLOCK, row * BLOCK : (row + 1) * BLOCK] = tile.T

    def step(k, carry):
        at = pl.ds(pl.multiple_of(k * BLOCK, BLOCK), BLOCK)
        base = pl.multiple_of(k * BLOCK, BLOCK)
        tiles = [
            out_ref[pl.ds(base + ROWS * t, ROWS), at] for t in range(BLOCK // ROWS)
        ]
        for t, tile in enumerate(block_inverse(tiles)):
            diag_ref[pl.ds(ROWS * t, ROWS), :] = tile
        diag = diag_ref[...]
        panel = jnp.dot(
            left_parts(diag),
            right_parts(out_ref[at, :], 0),
            preferred_element_type=jnp.float32,
        )
        out_ref[at, :] = panel
        out_ref[at, at] = diag
        right_ref[...] = right_parts(out_ref[at, :], 0)
        diag_right = right_parts(diag, 1)

        def update(i, carry):
            rows = pl.ds(pl.multiple_of(i * BLOCK, BLOCK), BLOCK)
            lower = dot_nt(left_parts(out_ref[rows, at]), diag_right)
            out_ref[rows, at] = jnp.zeros((BLOCK, BLOCK), jnp.float32)
            out_ref[rows, :] -= jnp.dot(
                left_parts(lower), right_ref[...], preferred_element_type=jnp.float32
            )
            return carry

        lax.fori_loop(k + 1, blocks, update, 0)
        return carry

    lax.fori_loop(0, blocks, step, 0)
    row = lax.broadcasted_iota(jnp.int32, (BLOCK, out_ref.shape[1]), 0)
    col = lax.broadcasted_iota(jnp.int32, (BLOCK, out_ref.shape[1]), 1)

    def clear(i, carry):
        rows = pl.ds(pl.multiple_of(i * BLOCK, BLOCK), BLOCK)
        out_ref[rows, :] = jnp.where(col <= row + i * BLOCK, out_ref[rows, :], 0.0)
        return carry

    lax.fori_loop(0, blocks, clear, 0)


def inverse_factor(gram):
    n = 2 * gram.shape[0]
    return pl.pallas_call(
        factor_kernel,
        out_shape=jax.ShapeDtypeStruct((n, n), jnp.float32),
        in_specs=[pl.BlockSpec(memory_space=pltpu.VMEM)],
        out_specs=pl.BlockSpec(memory_space=pltpu.VMEM),
        scratch_shapes=[
            pltpu.VMEM((BLOCK, BLOCK), jnp.float32),
            pltpu.VMEM((3 * BLOCK, n), jnp.bfloat16),
        ],
        compiler_params=pltpu.CompilerParams(vmem_limit_bytes=32 * 1024 * 1024),
        cost_estimate=pl.CostEstimate(
            flops=60 * n * n * n, bytes_accessed=8 * n * n, transcendentals=n
        ),
    )(gram)


def pack(top, bottom, tiles):
    return jnp.concatenate([top[:, : tiles * BLOCK], bottom[:, : bottom.shape[1] + BLOCK - tiles * BLOCK]], 1)


def swap(x, band, bit):
    return lax.ppermute(x, "band", [(i, i ^ bit) for i in range(band)])


def body(basis, panel):
    grid, band = lax.axis_size("grid"), lax.axis_size("band")
    at_grid, at_band = lax.axis_index("grid"), lax.axis_index("band")
    n_grid = panel.shape[1] * grid
    rows_q = basis.shape[0]
    rows_p = panel.shape[0]
    n_panel = rows_p * band
    blocks = n_panel // BLOCK
    share_q, share_b = rows_q // grid, BLOCK // grid
    panel_all = lax.all_gather(panel, "band", axis=0, tiled=True)
    top = lax.dynamic_slice_in_dim(panel_all, at_band * BLOCK, BLOCK, 0)
    bottom = lax.dynamic_slice_in_dim(panel_all, (blocks - 1 - at_band) * BLOCK, BLOCK, 0)
    stacked = jnp.concatenate(
        [x.reshape(grid, x.shape[0] // grid, -1) for x in (basis, top, bottom)], 1
    ).reshape(rows_q + 2 * BLOCK, -1)
    both = tdot(stacked, panel_all)
    mine = lax.psum_scatter(both, "grid", scatter_dimension=0, tiled=True) / n_grid
    coeffs = lax.all_gather(mine[:share_q], "grid", axis=0, tiled=True)
    by_block = coeffs.reshape(rows_q, blocks, grid, share_b)
    picked = lax.dynamic_index_in_dim(by_block, at_grid, 2, keepdims=False)
    square = cdot(picked.reshape(rows_q, blocks * share_b), coeffs)
    square = square.reshape(blocks, share_b, n_panel)
    packed = jnp.concatenate(
        [pack(square[b], square[blocks - 1 - b], b + 1) for b in range(band)], 0
    )
    packed = lax.psum_scatter(packed, "band", scatter_dimension=0, tiled=True)
    mine_top = mine[share_q : share_q + share_b]
    mine_bottom = mine[share_q + share_b :]
    mine_packed = lax.switch(
        at_band, [functools.partial(pack, tiles=b + 1) for b in range(band)], mine_top, mine_bottom
    )
    gram = lax.all_gather(mine_packed - packed, ("band", "grid"), axis=0, tiled=True)

    bits = [1 << i for i in range(band.bit_length() - 1)]
    odd = at_band % 2

    def removed_rows(which):
        cols = [
            lax.dynamic_slice_in_dim(coeffs, (which + i) * rows_p, rows_p, 1)
            for i in range(0, band, 2)
        ]
        return cdot(jnp.concatenate(cols, 1), basis).reshape(band // 2, rows_p, -1)

    kept = removed_rows(odd) + swap(removed_rows(1 - odd), band, 1)
    for bit in bits[1:]:
        halves_of = kept.reshape(-1, 2, rows_p, kept.shape[-1])
        side = (at_band // bit) % 2
        sent = lax.dynamic_index_in_dim(halves_of, 1 - side, 1, keepdims=False)
        kept = lax.dynamic_index_in_dim(halves_of, side, 1, keepdims=False) + swap(sent, band, bit)
    projected = panel - kept.reshape(panel.shape)
    projected, gram = lax.optimization_barrier((projected, gram))
    others = [projected] + [swap(projected, band, d) for d in range(1, band)]
    inverse = inverse_factor(gram)
    inverse_rows = lax.dynamic_slice_in_dim(inverse, at_band * rows_p, rows_p, 0)
    new_panel = 0.0
    for d, rows in enumerate(others):
        cols = lax.dynamic_slice_in_dim(inverse_rows, (at_band ^ d) * rows_p, rows_p, 1)
        new_panel = new_panel + jnp.dot(cols, rows, precision=lax.Precision.HIGH)
    return (new_panel, coeffs)


def solution(mesh):
    placed = (P("band", "grid"), P("band", "grid"))
    return jax.shard_map(
        body,
        mesh=mesh,
        in_specs=placed,
        out_specs=(P("band", "grid"), P("band", None)),
        check_vma=False,
    )
```

```python
import functools

import jax
import jax.numpy as jnp
from jax import lax
from jax.experimental import pallas as pl
from jax.experimental.pallas import tpu as pltpu
from jax.sharding import PartitionSpec as P

BLOCK = 128
ROWS = 8


def tdot(left, right):
    return lax.dot_general(
        left,
        right,
        (((1,), (1,)), ((), ())),
        precision=lax.Precision.HIGH,
        preferred_element_type=jnp.float32,
    )


def cdot(left, right):
    return lax.dot_general(
        left,
        right,
        (((0,), (0,)), ((), ())),
        precision=lax.Precision.HIGH,
        preferred_element_type=jnp.float32,
    )


def halves(x):
    high = x.astype(jnp.bfloat16)
    low = (x - high.astype(jnp.float32)).astype(jnp.bfloat16)
    return high, low


def left_parts(x):
    high, low = halves(x)
    return jnp.concatenate([high, high, low], 1)


def right_parts(x, axis):
    high, low = halves(x)
    return jnp.concatenate([high, low, high], axis)


def dot_nt(left, right):
    return lax.dot_general(
        left, right, (((1,), (1,)), ((), ())), preferred_element_type=jnp.float32
    )


def block_inverse(tiles):
    lanes = lax.broadcasted_iota(jnp.int32, (ROWS, BLOCK), 1)
    subs = lax.broadcasted_iota(jnp.int32, (ROWS, BLOCK), 0)
    shape = (ROWS, BLOCK)
    tiles = list(tiles)
    count = len(tiles)
    done = []
    for t in range(count):
        tile = tiles[t]
        base = ROWS * t
        here = (lanes >= base) & (lanes < base + ROWS)
        cols = [jnp.broadcast_to(tile[:, base + q : base + q + 1], shape) for q in range(ROWS)]
        entry = {
            (p, q): jnp.broadcast_to(cols[q][p : p + 1, :], shape)
            for q in range(ROWS)
            for p in range(q, ROWS)
        }
        start = jnp.where(here, jnp.where(lanes - base == subs, 1.0, 0.0), tile)
        rows = [jnp.broadcast_to(start[p : p + 1, :], shape) for p in range(ROWS)]
        unit = {}
        root = []
        scaled = []
        for q in range(ROWS):
            inv_root = lax.rsqrt(entry[q, q])
            inv = inv_root * inv_root
            root.append(inv_root)
            scaled.append(inv)
            for p in range(q + 1, ROWS):
                unit[p, q] = entry[p, q] * inv
            for p in range(q + 1, ROWS):
                for s in range(q + 1, p + 1):
                    entry[p, s] = entry[p, s] - unit[p, q] * entry[s, q]
                rows[p] = rows[p] - unit[p, q] * rows[q]
        out = rows[0] * root[0]
        for p in range(1, ROWS):
            out = jnp.where(subs == p, rows[p] * root[p], out)
        done.append(jnp.where(lanes <= base + subs, out, 0.0))
        if t + 1 < count:
            back = [rows[p] * scaled[p] for p in range(ROWS)]
            for p in range(ROWS - 1, 0, -1):
                for q in range(p):
                    back[q] = back[q] - unit[p, q] * back[p]
            for u in range(t + 1, count):
                old = tiles[u]
                new = jnp.where(here, 0.0, old)
                for p in range(ROWS):
                    new = new - jnp.broadcast_to(old[:, base + p : base + p + 1], shape) * back[p]
                tiles[u] = new
    return done


def factor_kernel(gram_ref, out_ref, diag_ref, right_ref):
    blocks = out_ref.shape[0] // BLOCK
    for pair in range(blocks // 2):
        rows = slice(pair * BLOCK, (pair + 1) * BLOCK)
        for row, tiles, first in ((pair, pair + 1, 0), (blocks - 1 - pair, blocks - pair, pair + 1)):
            for col in range(tiles):
                tile = gram_ref[rows, (first + col) * BLOCK : (first + col + 1) * BLOCK]
                out_ref[row * BLOCK : (row + 1) * BLOCK, col * BLOCK : (col + 1) * BLOCK] = tile
                if col < row:
                    out_ref[col * BLOCK : (col + 1) * BLOCK, row * BLOCK : (row + 1) * BLOCK] = tile.T

    def step(k, carry):
        at = pl.ds(pl.multiple_of(k * BLOCK, BLOCK), BLOCK)
        base = pl.multiple_of(k * BLOCK, BLOCK)
        tiles = [
            out_ref[pl.ds(base + ROWS * t, ROWS), at] for t in range(BLOCK // ROWS)
        ]
        for t, tile in enumerate(block_inverse(tiles)):
            diag_ref[pl.ds(ROWS * t, ROWS), :] = tile
        diag = diag_ref[...]
        panel = jnp.dot(
            left_parts(diag),
            right_parts(out_ref[at, :], 0),
            preferred_element_type=jnp.float32,
        )
        out_ref[at, :] = panel
        out_ref[at, at] = diag
        right_ref[...] = right_parts(out_ref[at, :], 0)
        diag_right = right_parts(diag, 1)

        def update(i, carry):
            rows = pl.ds(pl.multiple_of(i * BLOCK, BLOCK), BLOCK)
            lower = dot_nt(left_parts(out_ref[rows, at]), diag_right)
            out_ref[rows, at] = jnp.zeros((BLOCK, BLOCK), jnp.float32)
            out_ref[rows, :] -= jnp.dot(
                left_parts(lower), right_ref[...], preferred_element_type=jnp.float32
            )
            return carry

        lax.fori_loop(k + 1, blocks, update, 0)
        return carry

    lax.fori_loop(0, blocks, step, 0)
    row = lax.broadcasted_iota(jnp.int32, (BLOCK, out_ref.shape[1]), 0)
    col = lax.broadcasted_iota(jnp.int32, (BLOCK, out_ref.shape[1]), 1)

    def clear(i, carry):
        rows = pl.ds(pl.multiple_of(i * BLOCK, BLOCK), BLOCK)
        out_ref[rows, :] = jnp.where(col <= row + i * BLOCK, out_ref[rows, :], 0.0)
        return carry

    lax.fori_loop(0, blocks, clear, 0)


def inverse_factor(gram):
    n = 2 * gram.shape[0]
    return pl.pallas_call(
        factor_kernel,
        out_shape=jax.ShapeDtypeStruct((n, n), jnp.float32),
        in_specs=[pl.BlockSpec(memory_space=pltpu.VMEM)],
        out_specs=pl.BlockSpec(memory_space=pltpu.VMEM),
        scratch_shapes=[
            pltpu.VMEM((BLOCK, BLOCK), jnp.float32),
            pltpu.VMEM((3 * BLOCK, n), jnp.bfloat16),
        ],
        compiler_params=pltpu.CompilerParams(vmem_limit_bytes=32 * 1024 * 1024),
        cost_estimate=pl.CostEstimate(
            flops=60 * n * n * n, bytes_accessed=8 * n * n, transcendentals=n
        ),
    )(gram)


def pack(top, bottom, tiles):
    return jnp.concatenate([top[:, : tiles * BLOCK], bottom[:, : bottom.shape[1] + BLOCK - tiles * BLOCK]], 1)


def swap(x, band, bit):
    return lax.ppermute(x, "band", [(i, i ^ bit) for i in range(band)])


def body(basis, panel):
    grid, band = lax.axis_size("grid"), lax.axis_size("band")
    at_grid, at_band = lax.axis_index("grid"), lax.axis_index("band")
    n_grid = panel.shape[1] * grid
    rows_q = basis.shape[0]
    rows_p = panel.shape[0]
    n_panel = rows_p * band
    blocks = n_panel // BLOCK
    share_q, share_b = rows_q // grid, BLOCK // grid
    panel_all = lax.all_gather(panel, "band", axis=0, tiled=True)
    top = lax.dynamic_slice_in_dim(panel_all, at_band * BLOCK, BLOCK, 0)
    bottom = lax.dynamic_slice_in_dim(panel_all, (blocks - 1 - at_band) * BLOCK, BLOCK, 0)
    stacked = jnp.concatenate(
        [x.reshape(grid, x.shape[0] // grid, -1) for x in (basis, top, bottom)], 1
    ).reshape(rows_q + 2 * BLOCK, -1)
    both = tdot(stacked, panel_all)
    mine = lax.psum_scatter(both, "grid", scatter_dimension=0, tiled=True) / n_grid
    coeffs = lax.all_gather(mine[:share_q], "grid", axis=0, tiled=True)
    by_block = coeffs.reshape(rows_q, blocks, grid, share_b)
    picked = lax.dynamic_index_in_dim(by_block, at_grid, 2, keepdims=False)
    square = cdot(picked.reshape(rows_q, blocks * share_b), coeffs)
    square = square.reshape(blocks, share_b, n_panel)
    packed = jnp.concatenate(
        [pack(square[b], square[blocks - 1 - b], b + 1) for b in range(band)], 0
    )
    packed = lax.psum_scatter(packed, "band", scatter_dimension=0, tiled=True)
    mine_top = mine[share_q : share_q + share_b]
    mine_bottom = mine[share_q + share_b :]
    mine_packed = lax.switch(
        at_band, [functools.partial(pack, tiles=b + 1) for b in range(band)], mine_top, mine_bottom
    )
    bits = [1 << i for i in range(band.bit_length() - 1)]
    odd = at_band % 2

    def removed_rows(which):
        cols = [
            lax.dynamic_slice_in_dim(coeffs, (which + i) * rows_p, rows_p, 1)
            for i in range(0, band, 2)
        ]
        return cdot(jnp.concatenate(cols, 1), basis).reshape(band // 2, rows_p, -1)

    kept = removed_rows(odd) + swap(removed_rows(1 - odd), band, 1)
    for bit in bits[1:]:
        halves_of = kept.reshape(-1, 2, rows_p, kept.shape[-1])
        side = (at_band // bit) % 2
        sent = lax.dynamic_index_in_dim(halves_of, 1 - side, 1, keepdims=False)
        sent, packed = lax.optimization_barrier((sent, packed))
        kept = lax.dynamic_index_in_dim(halves_of, side, 1, keepdims=False) + swap(sent, band, bit)
    gram = lax.all_gather(mine_packed - packed, "grid", axis=0, tiled=True)
    gram = lax.all_gather(gram, "band", axis=0, tiled=True)
    projected = panel - kept.reshape(panel.shape)
    projected, gram = lax.optimization_barrier((projected, gram))
    others = [projected] + [swap(projected, band, d) for d in range(1, band)]
    inverse = inverse_factor(gram)
    inverse_rows = lax.dynamic_slice_in_dim(inverse, at_band * rows_p, rows_p, 0)
    new_panel = 0.0
    for d, rows in enumerate(others):
        cols = lax.dynamic_slice_in_dim(inverse_rows, (at_band ^ d) * rows_p, rows_p, 1)
        new_panel = new_panel + jnp.dot(cols, rows, precision=lax.Precision.HIGH)
    return (new_panel, coeffs)


def solution(mesh):
    placed = (P("band", "grid"), P("band", "grid"))
    return jax.shard_map(
        body,
        mesh=mesh,
        in_specs=placed,
        out_specs=(P("band", "grid"), P("band", None)),
        check_vma=False,
    )
```

```python
import functools

import jax
import jax.numpy as jnp
from jax import lax
from jax.experimental import pallas as pl
from jax.experimental.pallas import tpu as pltpu
from jax.sharding import PartitionSpec as P

BLOCK = 128
ROWS = 8


def tdot(left, right):
    return lax.dot_general(
        left,
        right,
        (((1,), (1,)), ((), ())),
        precision=lax.Precision.HIGH,
        preferred_element_type=jnp.float32,
    )


def cdot(left, right):
    return lax.dot_general(
        left,
        right,
        (((0,), (0,)), ((), ())),
        precision=lax.Precision.HIGH,
        preferred_element_type=jnp.float32,
    )


def halves(x):
    high = x.astype(jnp.bfloat16)
    low = (x - high.astype(jnp.float32)).astype(jnp.bfloat16)
    return high, low


def left_parts(x):
    high, low = halves(x)
    return jnp.concatenate([high, high, low], 1)


def right_parts(x, axis):
    high, low = halves(x)
    return jnp.concatenate([high, low, high], axis)


def dot_nt(left, right):
    return lax.dot_general(
        left, right, (((1,), (1,)), ((), ())), preferred_element_type=jnp.float32
    )


def block_inverse(tiles):
    lanes = lax.broadcasted_iota(jnp.int32, (ROWS, BLOCK), 1)
    subs = lax.broadcasted_iota(jnp.int32, (ROWS, BLOCK), 0)
    shape = (ROWS, BLOCK)
    tiles = list(tiles)
    count = len(tiles)
    done = []
    for t in range(count):
        tile = tiles[t]
        base = ROWS * t
        here = (lanes >= base) & (lanes < base + ROWS)
        cols = [jnp.broadcast_to(tile[:, base + q : base + q + 1], shape) for q in range(ROWS)]
        entry = {
            (p, q): jnp.broadcast_to(cols[q][p : p + 1, :], shape)
            for q in range(ROWS)
            for p in range(q, ROWS)
        }
        start = jnp.where(here, jnp.where(lanes - base == subs, 1.0, 0.0), tile)
        rows = [jnp.broadcast_to(start[p : p + 1, :], shape) for p in range(ROWS)]
        unit = {}
        root = []
        scaled = []
        for q in range(ROWS):
            inv_root = lax.rsqrt(entry[q, q])
            inv = inv_root * inv_root
            root.append(inv_root)
            scaled.append(inv)
            for p in range(q + 1, ROWS):
                unit[p, q] = entry[p, q] * inv
            for p in range(q + 1, ROWS):
                for s in range(q + 1, p + 1):
                    entry[p, s] = entry[p, s] - unit[p, q] * entry[s, q]
                rows[p] = rows[p] - unit[p, q] * rows[q]
        out = rows[0] * root[0]
        for p in range(1, ROWS):
            out = jnp.where(subs == p, rows[p] * root[p], out)
        done.append(jnp.where(lanes <= base + subs, out, 0.0))
        if t + 1 < count:
            back = [rows[p] * scaled[p] for p in range(ROWS)]
            for p in range(ROWS - 1, 0, -1):
                for q in range(p):
                    back[q] = back[q] - unit[p, q] * back[p]
            for u in range(t + 1, count):
                old = tiles[u]
                new = jnp.where(here, 0.0, old)
                for p in range(ROWS):
                    new = new - jnp.broadcast_to(old[:, base + p : base + p + 1], shape) * back[p]
                tiles[u] = new
    return done


def factor_kernel(gram_ref, out_ref, diag_ref, right_ref):
    blocks = out_ref.shape[0] // BLOCK
    for pair in range(blocks // 2):
        rows = slice(pair * BLOCK, (pair + 1) * BLOCK)
        for row, tiles, first in ((pair, pair + 1, 0), (blocks - 1 - pair, blocks - pair, pair + 1)):
            for col in range(tiles):
                tile = gram_ref[rows, (first + col) * BLOCK : (first + col + 1) * BLOCK]
                out_ref[row * BLOCK : (row + 1) * BLOCK, col * BLOCK : (col + 1) * BLOCK] = tile
                if col < row:
                    out_ref[col * BLOCK : (col + 1) * BLOCK, row * BLOCK : (row + 1) * BLOCK] = tile.T

    def step(k, carry):
        at = pl.ds(pl.multiple_of(k * BLOCK, BLOCK), BLOCK)
        base = pl.multiple_of(k * BLOCK, BLOCK)
        tiles = [
            out_ref[pl.ds(base + ROWS * t, ROWS), at] for t in range(BLOCK // ROWS)
        ]
        for t, tile in enumerate(block_inverse(tiles)):
            diag_ref[pl.ds(ROWS * t, ROWS), :] = tile
        diag = diag_ref[...]
        panel = jnp.dot(
            left_parts(diag),
            right_parts(out_ref[at, :], 0),
            preferred_element_type=jnp.float32,
        )
        out_ref[at, :] = panel
        out_ref[at, at] = diag
        right_ref[...] = right_parts(out_ref[at, :], 0)
        diag_right = right_parts(diag, 1)

        def update(i, carry):
            rows = pl.ds(pl.multiple_of(i * BLOCK, BLOCK), BLOCK)
            lower = dot_nt(left_parts(out_ref[rows, at]), diag_right)
            out_ref[rows, at] = jnp.zeros((BLOCK, BLOCK), jnp.float32)
            out_ref[rows, :] -= jnp.dot(
                left_parts(lower), right_ref[...], preferred_element_type=jnp.float32
            )
            return carry

        lax.fori_loop(k + 1, blocks, update, 0)
        return carry

    lax.fori_loop(0, blocks, step, 0)
    row = lax.broadcasted_iota(jnp.int32, (BLOCK, out_ref.shape[1]), 0)
    col = lax.broadcasted_iota(jnp.int32, (BLOCK, out_ref.shape[1]), 1)

    def clear(i, carry):
        rows = pl.ds(pl.multiple_of(i * BLOCK, BLOCK), BLOCK)
        out_ref[rows, :] = jnp.where(col <= row + i * BLOCK, out_ref[rows, :], 0.0)
        return carry

    lax.fori_loop(0, blocks, clear, 0)


def inverse_factor(gram):
    n = 2 * gram.shape[0]
    return pl.pallas_call(
        factor_kernel,
        out_shape=jax.ShapeDtypeStruct((n, n), jnp.float32),
        in_specs=[pl.BlockSpec(memory_space=pltpu.VMEM)],
        out_specs=pl.BlockSpec(memory_space=pltpu.VMEM),
        scratch_shapes=[
            pltpu.VMEM((BLOCK, BLOCK), jnp.float32),
            pltpu.VMEM((3 * BLOCK, n), jnp.bfloat16),
        ],
        compiler_params=pltpu.CompilerParams(vmem_limit_bytes=32 * 1024 * 1024),
        cost_estimate=pl.CostEstimate(
            flops=60 * n * n * n, bytes_accessed=8 * n * n, transcendentals=n
        ),
    )(gram)


def pack(top, bottom, tiles):
    return jnp.concatenate([top[:, : tiles * BLOCK], bottom[:, : bottom.shape[1] + BLOCK - tiles * BLOCK]], 1)


def swap(x, band, bit):
    return lax.ppermute(x, "band", [(i, i ^ bit) for i in range(band)])


def body(basis, panel):
    grid, band = lax.axis_size("grid"), lax.axis_size("band")
    at_grid, at_band = lax.axis_index("grid"), lax.axis_index("band")
    n_grid = panel.shape[1] * grid
    rows_q = basis.shape[0]
    rows_p = panel.shape[0]
    n_panel = rows_p * band
    blocks = n_panel // BLOCK
    share_q, share_b = rows_q // grid, BLOCK // grid
    panel_all = lax.all_gather(panel, "band", axis=0, tiled=True)
    top = lax.dynamic_slice_in_dim(panel_all, at_band * BLOCK, BLOCK, 0)
    bottom = lax.dynamic_slice_in_dim(panel_all, (blocks - 1 - at_band) * BLOCK, BLOCK, 0)
    stacked = jnp.concatenate(
        [x.reshape(grid, x.shape[0] // grid, -1) for x in (basis, top, bottom)], 1
    ).reshape(rows_q + 2 * BLOCK, -1)
    both = tdot(stacked, panel_all)
    mine = lax.psum_scatter(both, "grid", scatter_dimension=0, tiled=True) / n_grid
    coeffs = lax.all_gather(mine[:share_q], "grid", axis=0, tiled=True)
    by_block = coeffs.reshape(rows_q, blocks, grid, share_b)
    picked = lax.dynamic_index_in_dim(by_block, at_grid, 2, keepdims=False)
    square = cdot(picked.reshape(rows_q, blocks * share_b), coeffs)
    square = square.reshape(blocks, share_b, n_panel)
    packed = jnp.concatenate(
        [pack(square[b], square[blocks - 1 - b], b + 1) for b in range(band)], 0
    )
    packed = lax.psum_scatter(packed, "band", scatter_dimension=0, tiled=True)
    mine_top = mine[share_q : share_q + share_b]
    mine_bottom = mine[share_q + share_b :]
    mine_packed = lax.switch(
        at_band, [functools.partial(pack, tiles=b + 1) for b in range(band)], mine_top, mine_bottom
    )
    bits = [1 << i for i in range(band.bit_length() - 1)]
    odd = at_band % 2

    def removed_rows(which):
        cols = [
            lax.dynamic_slice_in_dim(coeffs, (which + i) * rows_p, rows_p, 1)
            for i in range(0, band, 2)
        ]
        return cdot(jnp.concatenate(cols, 1), basis).reshape(band // 2, rows_p, -1)

    kept = removed_rows(odd) + swap(removed_rows(1 - odd), band, 1)
    for bit in bits[1:]:
        halves_of = kept.reshape(-1, 2, rows_p, kept.shape[-1])
        side = (at_band // bit) % 2
        sent = lax.dynamic_index_in_dim(halves_of, 1 - side, 1, keepdims=False)
        held, packed = lax.optimization_barrier((sent, packed))
        kept = lax.dynamic_index_in_dim(halves_of, side, 1, keepdims=False) + swap(sent, band, bit)
    gram = lax.all_gather(mine_packed - packed, ("band", "grid"), axis=0, tiled=True)
    projected = panel - kept.reshape(panel.shape)
    projected, gram = lax.optimization_barrier((projected, gram))
    others = [projected] + [swap(projected, band, d) for d in range(1, band)]
    inverse = inverse_factor(gram)
    inverse_rows = lax.dynamic_slice_in_dim(inverse, at_band * rows_p, rows_p, 0)
    new_panel = 0.0
    for d, rows in enumerate(others):
        cols = lax.dynamic_slice_in_dim(inverse_rows, (at_band ^ d) * rows_p, rows_p, 1)
        new_panel = new_panel + jnp.dot(cols, rows, precision=lax.Precision.HIGH)
    return (new_panel, coeffs)


def solution(mesh):
    placed = (P("band", "grid"), P("band", "grid"))
    return jax.shard_map(
        body,
        mesh=mesh,
        in_specs=placed,
        out_specs=(P("band", "grid"), P("band", None)),
        check_vma=False,
    )
```
